32 devices in a mesh: parts: 2 (over x), frame: 2 (over core), tile: 8 (over z, y).
Axes of the slice: x: 2, y: 2, z: 4, core: 2. Of those that a mesh axis runs over, the one named last changes fastest.
Arguments:
- decoded_refs: bfloat16 [64, 96, 64, 256], P(('parts', 'frame'), None, 'tile'), parts along dimension 0, may hold values from -6 to 6
- current_frames: bfloat16 [16, 96, 64, 256], P(('parts', 'frame'), None, 'tile'), parts along dimension 0, may hold values from -6 to 6
- ref_pairs: int32 [16, 2], P('parts'), parts along dimension 0, may hold values from 0 to 31
- ref_slots: int32 [64], P('parts'), parts along dimension 0, may hold values from 0 to 31, each once
- frame_numbers: int32 [16], P('parts'), parts along dimension 0, may hold values from 0 to 31
- rate_weights: float32 [64], P('parts'), parts along dimension 0, may hold values from 0.5 to 4
- join_kernel: bfloat16 [3, 3, 96, 288], replicated, may hold values from -0.125 to 0.125
- out_kernel: bfloat16 [3, 3, 96, 96], replicated, may hold values from -0.21875 to 0.21875
Outputs:
- reconstruction: bfloat16 [16, 96, 64, 256], P(('parts', 'frame'), None, 'tile'), parts along dimension 0
- join_grad: float32 [6, 3, 96, 288], P('parts'), parts along dimension 0
- output_grad: float32 [6, 3, 96, 96], P('parts'), parts along dimension 0
The draws below stay inside these ranges and needn't reach their ends.
There are 2 independent parts, one for each index of `parts`. The reference program is written for one: setup_inputs(seed, part) draws one part's arguments, and reference() takes and returns one part's arrays. A program takes and returns all parts, laid end to end along the dimension named above; an argument that names none is the same for every part. Nothing has to cross between parts.
Inputs may be any that keep to these rules, and one draw needn't show every extreme that they name: `ref_pairs`: each B-frame names two decoded frames, possibly the same one. `ref_slots`: each slot holds exactly one decoded frame.
All inputs are finite; a program needn't handle non-finite values.
Results may differ from the reference program's by a relative error of at most 0.005.
Values may be sent and summed in bfloat16 or wider, within the bound.
A program may use at most 128 MiB of HBM per device.

```python
import math
import jax
import jax.numpy as jnp
from jax import lax

C = 96
COLS = 256
NB = 8
NREF = 32
GOP = 32
H = 64


def set_ends(array, stream_key, smallest, top_value):
    index_at = [jax.random.randint(jax.random.fold_in(stream_key, axis), (), 0, length) for axis, length in enumerate(array.shape)]
    main_axis = array.shape.index(max(array.shape))
    next_to = index_at[:main_axis] + [(index_at[main_axis] + 1) % array.shape[main_axis]] + index_at[main_axis + 1:]
    return array.at[tuple(index_at)].set(smallest).at[tuple(next_to)].set(top_value)


def levels(rng, shape, cuts, least, top_value):
    gain, own = 1.0, jax.random.fold_in(rng, 6)
    for dim, blocks in cuts:
        draws = jnp.exp(jax.random.uniform(jax.random.fold_in(own, dim), (blocks,), jnp.float32, least / len(cuts), top_value / len(cuts)))
        gain = gain * jnp.repeat(draws, shape[dim] // blocks).reshape([-1 if axis == dim else 1 for axis in range(len(shape))])
    return gain


def centred(own_key, shape, deviation, bound, split=(), held_as=jnp.bfloat16):
    entries = deviation * jax.random.normal(own_key, shape, jnp.float32)
    if split:
        entries = entries * levels(own_key, shape, split, -0.22, 0.18)
    return jnp.clip(entries, -bound, bound).astype(held_as)


def setup_inputs(seed: int = 0, part: int = 0) -> dict:
    splits = jax.random.split(jax.random.key(seed), 9)
    own_keys = jax.random.split(jax.random.fold_in(splits[8], part), 9)
    return {
        "decoded_refs": centred(own_keys[0], (NREF, C, H, COLS), 1.0, 6.0, ((0, 2), (2, 8))),
        "current_frames": centred(own_keys[1], (NB, C, H, COLS), 1.0, 6.0, ((0, 2), (2, 8))),
        "ref_pairs": set_ends(jax.random.randint(own_keys[2], (NB, 2), 0, NREF), jax.random.fold_in(own_keys[2], 1), 0, NREF - 1).astype(jnp.int32),
        "ref_slots": jax.random.permutation(own_keys[3], NREF).astype(jnp.int32),
        "frame_numbers": set_ends(jax.random.randint(own_keys[4], (NB,), 0, GOP), jax.random.fold_in(own_keys[4], 1), 0, GOP - 1).astype(jnp.int32),
        "rate_weights": jnp.clip(jnp.exp(jax.random.uniform(own_keys[5], (GOP,), jnp.float32, math.log(0.5), math.log(4.0))), 0.5, 4.0),
        "join_kernel": centred(splits[6], (3, 3, C, 3 * C), (27 * C) ** -0.5, 0.125),
        "out_kernel": centred(splits[7], (3, 3, C, C), (9 * C) ** -0.5, 0.21875),
    }


def sigmoid_grad(value):
    sigma = jax.nn.sigmoid(value)
    return sigma * (1.0 + value * (1.0 - sigma))

def apply_taps(padded, kernel, row_count, col_count):
    running = jnp.zeros((kernel.shape[2], row_count, col_count), jnp.float32)
    for row_tap in range(3):
        for col_tap in range(3):
            window = padded[:, row_tap:row_tap + row_count, col_tap:col_tap + col_count]
            running = running + jnp.einsum('oi,ihw->ohw', kernel[row_tap, col_tap], window)
    return running

def tap_grads(upstream, padded, row_count, col_count):
    pieces = []
    for row_tap in range(3):
        for col_tap in range(3):
            window = padded[:, row_tap:row_tap + row_count, col_tap:col_tap + col_count]
            pieces.append(jnp.einsum('ohw,ihw->oi', upstream, window))
    stacked = jnp.stack(pieces)
    return stacked.reshape((3, 3) + stacked.shape[1:])

def pad_frame(field):
    return jnp.pad(field, ((0, 0), (1, 1), (1, 1)))

def reference(decoded_refs, current_frames, ref_pairs, ref_slots, frame_numbers, rate_weights, join_kernel, out_kernel):
    row_count = current_frames.shape[2]
    col_count = current_frames.shape[3]
    join_full = join_kernel.astype(jnp.float32)
    out_full = out_kernel.astype(jnp.float32)

    def frame_step(index):
        slot_ids = ref_slots[ref_pairs[index]]
        stacked = jnp.concatenate([decoded_refs[slot_ids[0]], decoded_refs[slot_ids[1]], current_frames[index]], 0)
        stacked_pad = pad_frame(stacked.astype(jnp.float32))
        preact = apply_taps(stacked_pad, join_full, row_count, col_count)
        hidden = jax.nn.silu(preact).astype(jnp.bfloat16)
        hidden = lax.optimization_barrier(hidden).astype(jnp.float32)
        hidden_pad = pad_frame(hidden)
        recon = apply_taps(hidden_pad, out_full, row_count, col_count)
        rate_weight = rate_weights[frame_numbers[index]]
        residual = (2.0 * rate_weight * (recon - current_frames[index].astype(jnp.float32)) / (row_count * col_count)).astype(jnp.bfloat16)
        residual = lax.optimization_barrier(residual).astype(jnp.float32)
        output_part = tap_grads(residual, hidden_pad, row_count, col_count)
        residual_pad = pad_frame(residual)
        hidden_grad = jnp.zeros((out_full.shape[3], row_count, col_count), jnp.float32)
        for row_tap in range(3):
            for col_tap in range(3):
                window = residual_pad[:, 2 - row_tap:2 - row_tap + row_count, 2 - col_tap:2 - col_tap + col_count]
                hidden_grad = hidden_grad + jnp.einsum('oi,ohw->ihw', out_full[row_tap, col_tap], window)
        preact_grad = (hidden_grad * sigmoid_grad(preact)).astype(jnp.bfloat16)
        preact_grad = lax.optimization_barrier(preact_grad).astype(jnp.float32)
        join_part = tap_grads(preact_grad, stacked_pad, row_count, col_count)
        return (recon.astype(jnp.bfloat16), join_part, output_part)
    recon_all, join_parts, output_parts = lax.map(frame_step, jnp.arange(current_frames.shape[0], dtype=jnp.int32))
    return (recon_all, lax.optimization_barrier(jnp.sum(join_parts, 0)), lax.optimization_barrier(jnp.sum(output_parts, 0)))
```

```python
import functools

import jax
import jax.numpy as jnp
from jax import lax
from jax.experimental import pallas as pl
from jax.experimental.pallas import tpu as pltpu
from jax.sharding import PartitionSpec as P

MESH = pl.DeviceIdType.MESH
BF16 = jnp.bfloat16
F32 = jnp.float32


def partner(array, axis, stride):
    return lax.ppermute(array, axis, [(i, i ^ 1 << stride) for i in range(lax.axis_size(axis))])


def dot(a, b):
    return jnp.dot(a, b, preferred_element_type=F32)


def from_left(v):
    lane = lax.broadcasted_iota(jnp.int32, v.shape, 1)
    return jnp.where(lane == 0, 0.0, pltpu.roll(v, 1, 1))


def from_right(v):
    cols = v.shape[1]
    lane = lax.broadcasted_iota(jnp.int32, v.shape, 1)
    return jnp.where(lane == cols - 1, 0.0, pltpu.roll(v, cols - 1, 1))


def join_cols(v, ch):
    return from_left(v[:ch]) + v[ch : 2 * ch] + from_right(v[2 * ch :])


def kernel(
    groups, tiles, scale_cells, wt, x, kj, ko, kt,
    recon_out, gout,
    pre, hid, resq, pgq, part_s, part_r, acc, s0, r0, s1, r1,
    hs, hr, s0s, s0r, s1s, s1r, gs, gr, ps, pr,
):
    frames, rows, cin, cols = x.shape
    ch = cin // 3
    chunk = gout.shape[1]
    f = lax.axis_index("frame")
    t = lax.axis_index("tile")
    other = 1 - f
    has_up = t > 0
    has_down = t < tiles - 1

    barrier = pltpu.get_barrier_semaphore()
    pl.semaphore_signal(barrier, inc=1, device_id={"frame": other}, device_id_type=MESH)
    for k in range(1, tiles):
        pl.semaphore_signal(
            barrier, inc=1, device_id={"tile": lax.rem(t + k, tiles)}, device_id_type=MESH
        )
    pl.semaphore_wait(barrier, tiles)

    def exchange(stage, to_up, up_slot, to_down, down_slot):
        up = pltpu.make_async_remote_copy(
            src_ref=to_up, dst_ref=up_slot, send_sem=hs.at[stage, 0], recv_sem=hr.at[stage, 0],
            device_id={"tile": lax.max(t - 1, 0)}, device_id_type=MESH,
        )
        down = pltpu.make_async_remote_copy(
            src_ref=to_down, dst_ref=down_slot, send_sem=hs.at[stage, 1], recv_sem=hr.at[stage, 1],
            device_id={"tile": lax.min(t + 1, tiles - 1)}, device_id_type=MESH,
        )

        @pl.when(has_up)
        def _():
            up.start()

        @pl.when(has_down)
        def _():
            down.start()

        def arrive():
            @pl.when(has_up)
            def _():
                down.wait_recv()
                up.wait_send()

            @pl.when(has_down)
            def _():
                up.wait_recv()
                down.wait_send()

        return arrive

    edge = jnp.zeros((frames, ch, cols), BF16)

    @pl.when(jnp.logical_not(has_up))
    def _():
        part_r[0] = edge
        hid[:, 0] = edge
        resq[1, :, 0] = edge
        pgq[1, :, 0] = edge

    @pl.when(jnp.logical_not(has_down))
    def _():
        part_r[1] = edge
        hid[:, rows + 1] = edge
        resq[1, :, rows + 1] = edge
        pgq[1, :, rows + 1] = edge

    @pl.loop(0, frames)
    def _(b):
        part_s[0, b] = join_cols(dot(kj[:, 2 * cin :], x[b, 0]), ch).astype(BF16)
        part_s[1, b] = join_cols(dot(kj[:, :cin], x[b, rows - 1]), ch).astype(BF16)

    acc[...] = jnp.zeros_like(acc)
    arrive = exchange(0, part_s.at[0], part_r.at[1], part_s.at[1], part_r.at[0])

    def activate(b, r, v):
        pre[b, r] = v
        hid[b, r + 1] = (v * jax.nn.sigmoid(v)).astype(BF16)

    @pl.loop(0, frames)
    def _(b):
        pre[b, 0] = join_cols(dot(kj[:, cin:], x[b, 0:2].reshape(2 * cin, cols)), ch)
        pre[b, rows - 1] = join_cols(
            dot(kj[:, : 2 * cin], x[b, rows - 2 : rows].reshape(2 * cin, cols)), ch
        )
        for r in range(1, rows - 1):
            v = join_cols(dot(kj[...], x[b, r - 1 : r + 2].reshape(3 * cin, cols)), ch)
            activate(b, r, v)

    arrive()

    @pl.loop(0, frames)
    def _(b):
        activate(b, 0, pre[b, 0] + part_r[0, b].astype(F32))
        activate(b, rows - 1, pre[b, rows - 1] + part_r[1, b].astype(F32))

    arrive = exchange(1, hid.at[:, 1], hid.at[:, rows + 1], hid.at[:, rows], hid.at[:, 0])

    def shifted(buf, b, r, v):
        buf[0, b, r] = from_right(v).astype(BF16)
        buf[2, b, r] = from_left(v).astype(BF16)

    def reconstruct(b, r):
        v = join_cols(dot(ko[...], hid[b, r : r + 3].reshape(3 * ch, cols)), ch)
        recon_out[b, r] = v.astype(BF16)
        current = x[b, r, 2 * ch :].astype(F32)
        res = (2.0 * wt[b] * (v - current) / scale_cells).astype(BF16)
        resq[1, b, r + 1] = res
        shifted(resq, b, r + 1, res.astype(F32))

    @pl.loop(0, frames)
    def _(b):
        for r in range(1, rows - 1):
            reconstruct(b, r)

    arrive()

    @pl.loop(0, frames)
    def _(b):
        reconstruct(b, 0)
        reconstruct(b, rows - 1)

    arrive = exchange(
        2, resq.at[1, :, 1], resq.at[1, :, rows + 1], resq.at[1, :, rows], resq.at[1, :, 0]
    )

    def through(b, r):
        hg = join_cols(dot(kt[...], resq[1, b, r : r + 3].reshape(3 * ch, cols)), ch)
        v = pre[b, r]
        s = jax.nn.sigmoid(v)
        pg = (hg * (s * (1.0 + v * (1.0 - s)))).astype(BF16)
        pgq[1, b, r + 1] = pg
        shifted(pgq, b, r + 1, pg.astype(F32))

    @pl.loop(0, frames)
    def _(b):
        for r in range(1, rows - 1):
            through(b, r)

    arrive()

    @pl.loop(0, frames)
    def _(b):
        through(b, 0)
        through(b, rows - 1)

    arrive = exchange(
        3, pgq.at[1, :, 1], pgq.at[1, :, rows + 1], pgq.at[1, :, rows], pgq.at[1, :, 0]
    )

    def ends(buf):
        @pl.loop(0, frames)
        def _(b):
            for r in (0, rows + 1):
                shifted(buf, b, r, buf[1, b, r].astype(F32))

    def row_band(get):
        return jnp.concatenate([get(r) for r in range(rows)], axis=1)

    def taps(buf, b):
        return jnp.concatenate(
            [
                row_band(lambda r: buf[q, b, r + 2 - p])
                for p in range(3)
                for q in range(3)
            ],
            axis=0,
        )

    def tap_dot(a, b):
        return lax.dot_general(a, b, (((1,), (1,)), ((), ())), preferred_element_type=F32)

    span = 9 * ch
    width = cin + ch
    low = cin // 128 * 128

    ends(resq)

    @pl.loop(0, frames)
    def _(b):
        base = row_band(lambda r: hid[b, r + 1])
        base = jnp.concatenate([jnp.zeros((cin - low, rows * cols), BF16), base], axis=0)
        acc[:span, low:] += tap_dot(taps(resq, b), base)

    arrive()
    ends(pgq)

    @pl.loop(0, frames)
    def _(b):
        base = row_band(lambda r: x[b, r])
        base = jnp.concatenate([base, jnp.zeros((ch, rows * cols), BF16)], axis=0)
        acc[:span] += tap_dot(taps(pgq, b), base)

    def rows_of(index):
        return pl.ds(pl.multiple_of(index * chunk, 8), chunk)

    def remote(src, dst, send, recv, **where):
        return pltpu.make_async_remote_copy(
            src_ref=src, dst_ref=dst, send_sem=send, recv_sem=recv,
            device_id=where, device_id_type=MESH,
        )

    order = [lax.rem(t + k, tiles) for k in range(1, tiles)] + [t]
    sends = []
    for d in order:
        s0[d] = acc[rows_of(other * tiles + d)].astype(BF16)
    for d in order:
        c = remote(s0.at[d], r0.at[d], s0s.at[d], s0r.at[d], frame=other)
        c.start()
        sends.append(c)
    total = None
    for i, d in enumerate(order):
        sends[i].wait_recv()
        v = acc[rows_of(f * tiles + d)] + r0[d].astype(F32)
        if i == tiles - 1:
            total = v
            break
        s1[d] = v.astype(BF16)
        c = remote(s1.at[d], r1.at[t], s1s.at[d], s1r.at[t], tile=d)
        c.start()
        sends.append(c)
    for d in order[:-1]:
        remote(s1.at[d], r1.at[d], s1s.at[d], s1r.at[d], tile=d).wait_recv()
        total = total + r1[d].astype(F32)
    mine = f * tiles + t
    gout[mine] = total.astype(BF16)
    for d in order[:-1]:
        c = remote(gout.at[mine], gout.at[mine], gs.at[d], gr.at[t], tile=d)
        c.start()
        sends.append(c)
    across = []
    for d in [t] + [lax.rem(t + tiles - k, tiles) for k in range(1, tiles)]:
        slot = f * tiles + d
        if across:
            remote(gout.at[slot], gout.at[slot], gs.at[d], gr.at[d], tile=d).wait_recv()
        c = remote(gout.at[slot], gout.at[slot], ps.at[d], pr.at[d], frame=other)
        c.start()
        across.append(c)
        sends.append(c)
    for d in order:
        slot = other * tiles + d
        remote(gout.at[slot], gout.at[slot], ps.at[d], pr.at[d], frame=other).wait_recv()
    for c in sends:
        c.wait_send()


def run_kernel(weights, x, kj, ko, kt, height):
    groups, tiles = lax.axis_size("frame"), lax.axis_size("tile")
    frames, rows, cin, cols = x.shape
    ch = cin // 3
    count = groups * tiles
    chunk = -(-9 * ch // (count * 8)) * 8
    width = cin + ch
    vm = pl.BlockSpec(memory_space=pltpu.VMEM)
    dma = pltpu.SemaphoreType.DMA
    return pl.pallas_call(
        functools.partial(kernel, groups, tiles, float(height * cols)),
        out_shape=(
            jax.ShapeDtypeStruct((frames, rows, ch, cols), BF16),
            jax.ShapeDtypeStruct((count, chunk, width), BF16),
        ),
        in_specs=[pl.BlockSpec(memory_space=pltpu.SMEM)] + [vm] * 4,
        out_specs=(vm, vm),
        scratch_shapes=[
            pltpu.VMEM((frames, rows, ch, cols), F32),
            pltpu.VMEM((frames, rows + 2, ch, cols), BF16),
            pltpu.VMEM((3, frames, rows + 2, ch, cols), BF16),
            pltpu.VMEM((3, frames, rows + 2, ch, cols), BF16),
            pltpu.VMEM((2, frames, ch, cols), BF16),
            pltpu.VMEM((2, frames, ch, cols), BF16),
            pltpu.VMEM((count * chunk, width), F32),
        ]
        + [pltpu.VMEM((tiles, chunk, width), BF16)] * 4
        + [dma((4, 2))] * 2
        + [dma((tiles,))] * 8,
        compiler_params=pltpu.CompilerParams(
            collective_id=0, has_side_effects=True, vmem_limit_bytes=60 * 2**20
        ),
    )(weights, x, kj, ko, kt)


def on_device(
    decoded_refs,
    current_frames,
    ref_pairs,
    ref_slots,
    frame_numbers,
    rate_weights,
    join_kernel,
    out_kernel,
):
    local_refs = decoded_refs.shape[0]
    local_frames, channels, tile_rows, col_count = current_frames.shape
    group = lax.axis_index("frame")
    frame_range = jnp.arange(ref_slots.shape[0], dtype=jnp.int32)

    def pair_slots(which):
        pairs = lax.dynamic_slice_in_dim(ref_pairs, which * local_frames, local_frames, 0)
        return jnp.sum(jnp.where(pairs[:, :, None] == frame_range, ref_slots, 0), axis=-1).reshape(
            -1
        )

    mine = pair_slots(group)
    other = pair_slots(1 - group) - group * local_refs
    outgoing = jnp.take(decoded_refs, jnp.clip(other, 0, local_refs - 1), axis=0)
    incoming = partner(outgoing, "frame", 0)
    mine_local = mine - group * local_refs
    mine_held = (mine_local >= 0) & (mine_local < local_refs)
    own_tiles = jnp.take(decoded_refs, jnp.clip(mine_local, 0, local_refs - 1), axis=0)
    picked = jnp.where(mine_held[:, None, None, None], own_tiles, incoming)
    picked = picked.reshape(local_frames, 2 * channels, tile_rows, col_count)
    stacked = jnp.concatenate([picked, current_frames], axis=1).transpose(0, 2, 1, 3)
    height = tile_rows * lax.axis_size("tile")

    frames_here = lax.dynamic_slice_in_dim(frame_numbers, group * local_frames, local_frames, 0)
    gop_range = jnp.arange(rate_weights.shape[0], dtype=jnp.int32)
    weight_here = jnp.sum(jnp.where(frames_here[:, None] == gop_range, rate_weights, 0.0), axis=-1)

    kj = join_kernel.transpose(1, 2, 0, 3).reshape(3 * channels, 9 * channels)
    ko = out_kernel.transpose(1, 2, 0, 3).reshape(3 * channels, 3 * channels)
    kt = out_kernel[::-1, ::-1].transpose(1, 3, 0, 2).reshape(3 * channels, 3 * channels)
    recon, grads = run_kernel(weight_here, stacked, kj, ko, kt, height)
    grads = grads.reshape(-1, 4 * channels)[: 9 * channels].astype(F32)
    grads = grads.reshape(3, 3, channels, 4 * channels)
    return (
        recon.transpose(0, 2, 1, 3),
        grads[..., : 3 * channels],
        grads[..., 3 * channels :],
    )


def solution(mesh):
    placed = (
        P(("parts", "frame"), None, "tile", None),
        P(("parts", "frame"), None, "tile", None),
        P("parts", None),
        P("parts"),
        P("parts"),
        P("parts"),
        P(),
        P(),
    )
    return jax.shard_map(
        on_device,
        mesh=mesh,
        in_specs=placed,
        out_specs=(
            P(("parts", "frame"), None, "tile", None),
            P("parts", None, None, None),
            P("parts", None, None, None),
        ),
        check_vma=False,
    )
```

```python
import functools

import jax
import jax.numpy as jnp
from jax import lax
from jax.experimental import pallas as pl
from jax.experimental.pallas import tpu as pltpu
from jax.sharding import PartitionSpec as P

MESH = pl.DeviceIdType.MESH
BF16 = jnp.bfloat16
F32 = jnp.float32


def partner(array, axis, stride):
    return lax.ppermute(array, axis, [(i, i ^ 1 << stride) for i in range(lax.axis_size(axis))])


def dot(a, b):
    return jnp.dot(a, b, preferred_element_type=F32)


def from_left(v):
    lane = lax.broadcasted_iota(jnp.int32, v.shape, 1)
    return jnp.where(lane == 0, 0.0, pltpu.roll(v, 1, 1))


def from_right(v):
    cols = v.shape[1]
    lane = lax.broadcasted_iota(jnp.int32, v.shape, 1)
    return jnp.where(lane == cols - 1, 0.0, pltpu.roll(v, cols - 1, 1))


def join_cols(v, ch):
    return from_left(v[:ch]) + v[ch : 2 * ch] + from_right(v[2 * ch :])


def kernel(
    groups, tiles, scale_cells, wt, refs, current, kj_in, ko_in,
    recon_out, gout,
    x, kj, ko, kt, in_sem, pre, hid, resq, pgq, part_s, part_r, acc, s0, r0, s1, r1,
    hs, hr, s0s, s0r, s1s, s1r, gs, gr, ps, pr,
):
    frames, rows, cin, cols = x.shape
    ch = cin // 3
    chunk = gout.shape[1]
    f = lax.axis_index("frame")
    t = lax.axis_index("tile")
    other = 1 - f
    has_up = t > 0
    has_down = t < tiles - 1

    def load(b):
        return (
            pltpu.make_async_copy(refs.at[b], x.at[b, :, : 2 * ch], in_sem.at[b, 0]),
            pltpu.make_async_copy(current.at[b], x.at[b, :, 2 * ch :], in_sem.at[b, 1]),
        )

    for b in range(frames):
        for c in load(b):
            c.start()

    barrier = pltpu.get_barrier_semaphore()
    pl.semaphore_signal(barrier, inc=1, device_id={"frame": other}, device_id_type=MESH)
    for k in range(1, tiles):
        pl.semaphore_signal(
            barrier, inc=1, device_id={"tile": lax.rem(t + k, tiles)}, device_id_type=MESH
        )
    pl.semaphore_wait(barrier, tiles)

    def exchange(stage, b):
        if stage == 0:
            to_up, up_slot = part_s.at[0, b], part_r.at[1, b]
            to_down, down_slot = part_s.at[1, b], part_r.at[0, b]
        else:
            buf = (hid, resq.at[1], pgq.at[1])[stage - 1]
            to_up, up_slot = buf.at[b, 1], buf.at[b, rows + 1]
            to_down, down_slot = buf.at[b, rows], buf.at[b, 0]
        up = pltpu.make_async_remote_copy(
            src_ref=to_up, dst_ref=up_slot,
            send_sem=hs.at[stage, b, 0], recv_sem=hr.at[stage, b, 0],
            device_id={"tile": lax.max(t - 1, 0)}, device_id_type=MESH,
        )
        down = pltpu.make_async_remote_copy(
            src_ref=to_down, dst_ref=down_slot,
            send_sem=hs.at[stage, b, 1], recv_sem=hr.at[stage, b, 1],
            device_id={"tile": lax.min(t + 1, tiles - 1)}, device_id_type=MESH,
        )
        return up, down

    def send(stage, b):
        up, down = exchange(stage, b)

        @pl.when(has_up)
        def _():
            up.start()

        @pl.when(has_down)
        def _():
            down.start()

    def arrive(stage, b):
        up, down = exchange(stage, b)

        @pl.when(has_up)
        def _():
            down.wait_recv()
            up.wait_send()

        @pl.when(has_down)
        def _():
            up.wait_recv()
            down.wait_send()

    edge = jnp.zeros((frames, ch, cols), BF16)

    @pl.when(jnp.logical_not(has_up))
    def _():
        part_r[0] = edge
        hid[:, 0] = edge
        resq[1, :, 0] = edge
        pgq[1, :, 0] = edge

    @pl.when(jnp.logical_not(has_down))
    def _():
        part_r[1] = edge
        hid[:, rows + 1] = edge
        resq[1, :, rows + 1] = edge
        pgq[1, :, rows + 1] = edge

    for p in range(3):
        for q in range(3):
            kj[q * ch : (q + 1) * ch, p * cin : (p + 1) * cin] = kj_in[p, q]
            ko[q * ch : (q + 1) * ch, p * ch : (p + 1) * ch] = ko_in[p, q]
            flipped = ko_in[2 - p, 2 - q].astype(F32).T.astype(BF16)
            kt[q * ch : (q + 1) * ch, p * ch : (p + 1) * ch] = flipped

    @pl.loop(0, frames)
    def _(b):
        for c in load(b):
            c.wait()
        part_s[0, b] = join_cols(dot(kj[:, 2 * cin :], x[b, 0]), ch).astype(BF16)
        part_s[1, b] = join_cols(dot(kj[:, :cin], x[b, rows - 1]), ch).astype(BF16)
        send(0, b)

    acc[...] = jnp.zeros_like(acc)

    def activate(b, r, v):
        pre[b, r] = v
        hid[b, r + 1] = (v * jax.nn.sigmoid(v)).astype(BF16)

    @pl.loop(0, frames)
    def _(b):
        pre[b, 0] = join_cols(dot(kj[:, cin:], x[b, 0:2].reshape(2 * cin, cols)), ch)
        pre[b, rows - 1] = join_cols(
            dot(kj[:, : 2 * cin], x[b, rows - 2 : rows].reshape(2 * cin, cols)), ch
        )
        for r in range(1, rows - 1):
            v = join_cols(dot(kj[...], x[b, r - 1 : r + 2].reshape(3 * cin, cols)), ch)
            activate(b, r, v)
        arrive(0, b)
        activate(b, 0, pre[b, 0] + part_r[0, b].astype(F32))
        activate(b, rows - 1, pre[b, rows - 1] + part_r[1, b].astype(F32))
        send(1, b)

    def shifted(buf, b, r, v):
        buf[0, b, r] = from_right(v).astype(BF16)
        buf[2, b, r] = from_left(v).astype(BF16)

    def reconstruct(b, r):
        v = join_cols(dot(ko[...], hid[b, r : r + 3].reshape(3 * ch, cols)), ch)
        recon_out[b, r] = v.astype(BF16)
        target = x[b, r, 2 * ch :].astype(F32)
        res = (2.0 * wt[b] * (v - target) / scale_cells).astype(BF16)
        resq[1, b, r + 1] = res
        shifted(resq, b, r + 1, res.astype(F32))

    @pl.loop(0, frames)
    def _(b):
        for r in range(1, rows - 1):
            reconstruct(b, r)
        arrive(1, b)
        reconstruct(b, 0)
        reconstruct(b, rows - 1)
        send(2, b)

    def through(b, r):
        hg = join_cols(dot(kt[...], resq[1, b, r : r + 3].reshape(3 * ch, cols)), ch)
        v = pre[b, r]
        s = jax.nn.sigmoid(v)
        pg = (hg * (s * (1.0 + v * (1.0 - s)))).astype(BF16)
        pgq[1, b, r + 1] = pg
        shifted(pgq, b, r + 1, pg.astype(F32))

    @pl.loop(0, frames)
    def _(b):
        for r in range(1, rows - 1):
            through(b, r)
        arrive(2, b)
        through(b, 0)
        through(b, rows - 1)
        send(3, b)

    def ends(buf, b):
        for r in (0, rows + 1):
            shifted(buf, b, r, buf[1, b, r].astype(F32))

    def row_band(get):
        return jnp.concatenate([get(r) for r in range(rows)], axis=1)

    def taps(buf, b):
        return jnp.concatenate(
            [
                row_band(lambda r: buf[q, b, r + 2 - p])
                for p in range(3)
                for q in range(3)
            ],
            axis=0,
        )

    def tap_dot(a, b):
        return lax.dot_general(a, b, (((1,), (1,)), ((), ())), preferred_element_type=F32)

    span = 9 * ch
    width = cin + ch
    low = cin // 128 * 128

    @pl.loop(0, frames)
    def _(b):
        ends(resq, b)
        base = row_band(lambda r: hid[b, r + 1])
        base = jnp.concatenate([jnp.zeros((cin - low, rows * cols), BF16), base], axis=0)
        acc[:span, low:] += tap_dot(taps(resq, b), base)

    @pl.loop(0, frames)
    def _(b):
        arrive(3, b)
        ends(pgq, b)
        base = row_band(lambda r: x[b, r])
        base = jnp.concatenate([base, jnp.zeros((ch, rows * cols), BF16)], axis=0)
        acc[:span] += tap_dot(taps(pgq, b), base)

    def rows_of(index):
        return pl.ds(pl.multiple_of(index * chunk, 8), chunk)

    def remote(src, dst, send, recv, **where):
        return pltpu.make_async_remote_copy(
            src_ref=src, dst_ref=dst, send_sem=send, recv_sem=recv,
            device_id=where, device_id_type=MESH,
        )

    order = [lax.rem(t + k, tiles) for k in range(1, tiles)] + [t]
    sends = []
    for d in order:
        s0[d] = acc[rows_of(other * tiles + d)].astype(BF16)
    for d in order:
        c = remote(s0.at[d], r0.at[d], s0s.at[d], s0r.at[d], frame=other)
        c.start()
        sends.append(c)
    total = None
    for i, d in enumerate(order):
        sends[i].wait_recv()
        v = acc[rows_of(f * tiles + d)] + r0[d].astype(F32)
        if i == tiles - 1:
            total = v
            break
        s1[d] = v.astype(BF16)
        c = remote(s1.at[d], r1.at[t], s1s.at[d], s1r.at[t], tile=d)
        c.start()
        sends.append(c)
    for d in order[:-1]:
        remote(s1.at[d], r1.at[d], s1s.at[d], s1r.at[d], tile=d).wait_recv()
        total = total + r1[d].astype(F32)
    mine = f * tiles + t
    gout[mine] = total.astype(BF16)
    for d in order[:-1]:
        c = remote(gout.at[mine], gout.at[mine], gs.at[d], gr.at[t], tile=d)
        c.start()
        sends.append(c)
    across = []
    for d in [t] + [lax.rem(t + tiles - k, tiles) for k in range(1, tiles)]:
        slot = f * tiles + d
        if across:
            remote(gout.at[slot], gout.at[slot], gs.at[d], gr.at[d], tile=d).wait_recv()
        c = remote(gout.at[slot], gout.at[slot], ps.at[d], pr.at[d], frame=other)
        c.start()
        across.append(c)
        sends.append(c)
    for d in order:
        slot = other * tiles + d
        remote(gout.at[slot], gout.at[slot], ps.at[d], pr.at[d], frame=other).wait_recv()
    for c in sends:
        c.wait_send()


def run_kernel(weights, refs, current, join_kernel, out_kernel, height):
    groups, tiles = lax.axis_size("frame"), lax.axis_size("tile")
    frames, rows, ch, cols = current.shape
    cin = 3 * ch
    count = groups * tiles
    chunk = -(-9 * ch // (count * 8)) * 8
    width = cin + ch
    vm = pl.BlockSpec(memory_space=pltpu.VMEM)
    dma = pltpu.SemaphoreType.DMA
    return pl.pallas_call(
        functools.partial(kernel, groups, tiles, float(height * cols)),
        out_shape=(
            jax.ShapeDtypeStruct((frames, rows, ch, cols), BF16),
            jax.ShapeDtypeStruct((count, chunk, width), BF16),
        ),
        in_specs=[pl.BlockSpec(memory_space=pltpu.SMEM)]
        + [pl.BlockSpec(memory_space=pl.ANY)] * 2
        + [vm] * 2,
        out_specs=(vm, vm),
        scratch_shapes=[
            pltpu.VMEM((frames, rows, cin, cols), BF16),
            pltpu.VMEM((cin, 3 * cin), BF16),
            pltpu.VMEM((cin, cin), BF16),
            pltpu.VMEM((cin, cin), BF16),
            dma((frames, 2)),
            pltpu.VMEM((frames, rows, ch, cols), F32),
            pltpu.VMEM((frames, rows + 2, ch, cols), BF16),
            pltpu.VMEM((3, frames, rows + 2, ch, cols), BF16),
            pltpu.VMEM((3, frames, rows + 2, ch, cols), BF16),
            pltpu.VMEM((2, frames, ch, cols), BF16),
            pltpu.VMEM((2, frames, ch, cols), BF16),
            pltpu.VMEM((count * chunk, width), F32),
        ]
        + [pltpu.VMEM((tiles, chunk, width), BF16)] * 4
        + [dma((4, frames, 2))] * 2
        + [dma((tiles,))] * 8,
        compiler_params=pltpu.CompilerParams(
            collective_id=0, has_side_effects=True, vmem_limit_bytes=60 * 2**20
        ),
    )(weights, refs, current, join_kernel, out_kernel)


def on_device(
    decoded_refs,
    current_frames,
    ref_pairs,
    ref_slots,
    frame_numbers,
    rate_weights,
    join_kernel,
    out_kernel,
):
    local_refs = decoded_refs.shape[0]
    local_frames, channels, tile_rows, col_count = current_frames.shape
    group = lax.axis_index("frame")
    frame_range = jnp.arange(ref_slots.shape[0], dtype=jnp.int32)

    def pair_slots(which):
        pairs = lax.dynamic_slice_in_dim(ref_pairs, which * local_frames, local_frames, 0)
        return jnp.sum(jnp.where(pairs[:, :, None] == frame_range, ref_slots, 0), axis=-1).reshape(
            -1
        )

    mine = pair_slots(group)
    other = pair_slots(1 - group) - group * local_refs
    outgoing = jnp.take(decoded_refs, jnp.clip(other, 0, local_refs - 1), axis=0, mode="clip")
    incoming = partner(outgoing, "frame", 0)
    mine_local = mine - group * local_refs
    mine_held = (mine_local >= 0) & (mine_local < local_refs)
    own_tiles = jnp.take(decoded_refs, jnp.clip(mine_local, 0, local_refs - 1), axis=0, mode="clip")
    picked = jnp.where(mine_held[:, None, None, None], own_tiles, incoming)
    picked = picked.reshape(local_frames, 2 * channels, tile_rows, col_count)
    refs = picked.transpose(0, 2, 1, 3)
    current = current_frames.transpose(0, 2, 1, 3)
    height = tile_rows * lax.axis_size("tile")

    frames_here = lax.dynamic_slice_in_dim(frame_numbers, group * local_frames, local_frames, 0)
    gop_range = jnp.arange(rate_weights.shape[0], dtype=jnp.int32)
    weight_here = jnp.sum(jnp.where(frames_here[:, None] == gop_range, rate_weights, 0.0), axis=-1)

    recon, grads = run_kernel(weight_here, refs, current, join_kernel, out_kernel, height)
    grads = grads.reshape(-1, 4 * channels)[: 9 * channels].astype(F32)
    grads = grads.reshape(3, 3, channels, 4 * channels)
    return (
        recon.transpose(0, 2, 1, 3),
        grads[..., : 3 * channels],
        grads[..., 3 * channels :],
    )


def solution(mesh):
    placed = (
        P(("parts", "frame"), None, "tile", None),
        P(("parts", "frame"), None, "tile", None),
        P("parts", None),
        P("parts"),
        P("parts"),
        P("parts"),
        P(),
        P(),
    )
    return jax.shard_map(
        on_device,
        mesh=mesh,
        in_specs=placed,
        out_specs=(
            P(("parts", "frame"), None, "tile", None),
            P("parts", None, None, None),
            P("parts", None, None, None),
        ),
        check_vma=False,
    )
```

```python
import functools

import jax
import jax.numpy as jnp
from jax import lax
from jax.experimental import pallas as pl
from jax.experimental.pallas import tpu as pltpu
from jax.sharding import PartitionSpec as P

MESH = pl.DeviceIdType.MESH
BF16 = jnp.bfloat16
F32 = jnp.float32


def partner(array, axis, stride):
    return lax.ppermute(array, axis, [(i, i ^ 1 << stride) for i in range(lax.axis_size(axis))])


def dot(a, b):
    return jnp.dot(a, b, preferred_element_type=F32)


def from_left(v):
    lane = lax.broadcasted_iota(jnp.int32, v.shape, 1)
    return jnp.where(lane == 0, 0.0, pltpu.roll(v, 1, 1))


def from_right(v):
    cols = v.shape[1]
    lane = lax.broadcasted_iota(jnp.int32, v.shape, 1)
    return jnp.where(lane == cols - 1, 0.0, pltpu.roll(v, cols - 1, 1))


def join_cols(v, ch):
    return from_left(v[:ch]) + v[ch : 2 * ch] + from_right(v[2 * ch :])


def kernel(
    groups, tiles, scale_cells, wt, refs, current, kj_in, ko_in,
    recon_out, gout,
    x, kj, ko, kt, in_sem, pre, hid, resq, pgq, part_s, part_r, acc, s0, r0, s1, r1,
    hs, hr, s0s, s0r, s1s, s1r, gs, gr, ps, pr,
):
    frames, rows, cin, cols = x.shape
    ch = cin // 3
    chunk = gout.shape[1]
    f = lax.axis_index("frame")
    t = lax.axis_index("tile")
    other = 1 - f
    has_up = t > 0
    has_down = t < tiles - 1

    def load(b):
        return (
            pltpu.make_async_copy(refs.at[b], x.at[b, :, : 2 * ch], in_sem.at[b, 0]),
            pltpu.make_async_copy(current.at[b], x.at[b, :, 2 * ch :], in_sem.at[b, 1]),
        )

    for b in range(frames):
        for c in load(b):
            c.start()

    barrier = pltpu.get_barrier_semaphore()
    pl.semaphore_signal(barrier, inc=1, device_id={"frame": other}, device_id_type=MESH)
    for k in range(1, tiles):
        pl.semaphore_signal(
            barrier, inc=1, device_id={"tile": lax.rem(t + k, tiles)}, device_id_type=MESH
        )
    pl.semaphore_wait(barrier, tiles)

    def exchange(stage, b):
        if stage == 0:
            to_up, up_slot = part_s.at[0, b], part_r.at[1, b]
            to_down, down_slot = part_s.at[1, b], part_r.at[0, b]
        else:
            buf = (hid, resq.at[1], pgq.at[1])[stage - 1]
            to_up, up_slot = buf.at[b, 1], buf.at[b, rows + 1]
            to_down, down_slot = buf.at[b, rows], buf.at[b, 0]
        up = pltpu.make_async_remote_copy(
            src_ref=to_up, dst_ref=up_slot,
            send_sem=hs.at[stage, b, 0], recv_sem=hr.at[stage, b, 0],
            device_id={"tile": lax.max(t - 1, 0)}, device_id_type=MESH,
        )
        down = pltpu.make_async_remote_copy(
            src_ref=to_down, dst_ref=down_slot,
            send_sem=hs.at[stage, b, 1], recv_sem=hr.at[stage, b, 1],
            device_id={"tile": lax.min(t + 1, tiles - 1)}, device_id_type=MESH,
        )
        return up, down

    def send(stage, b):
        up, down = exchange(stage, b)

        @pl.when(has_up)
        def _():
            up.start()

        @pl.when(has_down)
        def _():
            down.start()

    def arrive(stage, b):
        up, down = exchange(stage, b)

        @pl.when(has_up)
        def _():
            down.wait_recv()
            up.wait_send()

        @pl.when(has_down)
        def _():
            up.wait_recv()
            down.wait_send()

    edge = jnp.zeros((frames, ch, cols), BF16)

    @pl.when(jnp.logical_not(has_up))
    def _():
        part_r[0] = edge
        hid[:, 0] = edge
        resq[1, :, 0] = edge
        pgq[1, :, 0] = edge

    @pl.when(jnp.logical_not(has_down))
    def _():
        part_r[1] = edge
        hid[:, rows + 1] = edge
        resq[1, :, rows + 1] = edge
        pgq[1, :, rows + 1] = edge

    for p in range(3):
        for q in range(3):
            kj[q * ch : (q + 1) * ch, p * cin : (p + 1) * cin] = kj_in[p, q]
            ko[q * ch : (q + 1) * ch, p * ch : (p + 1) * ch] = ko_in[p, q]
            flipped = ko_in[2 - p, 2 - q].astype(F32).T.astype(BF16)
            kt[q * ch : (q + 1) * ch, p * ch : (p + 1) * ch] = flipped

    @pl.loop(0, frames)
    def _(b):
        for c in load(b):
            c.wait()
        part_s[0, b] = join_cols(dot(kj[:, 2 * cin :], x[b, 0]), ch).astype(BF16)
        part_s[1, b] = join_cols(dot(kj[:, :cin], x[b, rows - 1]), ch).astype(BF16)
        send(0, b)

    acc[...] = jnp.zeros_like(acc)

    def activate(b, r, v):
        pre[b, r] = v
        hid[b, r + 1] = (v * jax.nn.sigmoid(v)).astype(BF16)

    @pl.loop(0, frames)
    def _(b):
        pre[b, 0] = join_cols(dot(kj[:, cin:], x[b, 0:2].reshape(2 * cin, cols)), ch)
        pre[b, rows - 1] = join_cols(
            dot(kj[:, : 2 * cin], x[b, rows - 2 : rows].reshape(2 * cin, cols)), ch
        )
        for r in range(1, rows - 1):
            v = join_cols(dot(kj[...], x[b, r - 1 : r + 2].reshape(3 * cin, cols)), ch)
            activate(b, r, v)
        arrive(0, b)
        activate(b, 0, pre[b, 0] + part_r[0, b].astype(F32))
        activate(b, rows - 1, pre[b, rows - 1] + part_r[1, b].astype(F32))
        send(1, b)

    def shifted(buf, b, r, v):
        buf[0, b, r] = from_right(v).astype(BF16)
        buf[2, b, r] = from_left(v).astype(BF16)

    def reconstruct(b, r):
        v = join_cols(dot(ko[...], hid[b, r : r + 3].reshape(3 * ch, cols)), ch)
        recon_out[b, r] = v.astype(BF16)
        target = x[b, r, 2 * ch :].astype(F32)
        res = (2.0 * wt[b] * (v - target) / scale_cells).astype(BF16)
        resq[1, b, r + 1] = res
        shifted(resq, b, r + 1, res.astype(F32))

    @pl.loop(0, frames)
    def _(b):
        for r in range(1, rows - 1):
            reconstruct(b, r)
        arrive(1, b)
        reconstruct(b, 0)
        reconstruct(b, rows - 1)
        send(2, b)

    def through(b, r):
        hg = join_cols(dot(kt[...], resq[1, b, r : r + 3].reshape(3 * ch, cols)), ch)
        v = pre[b, r]
        s = jax.nn.sigmoid(v)
        pg = (hg * (s * (1.0 + v * (1.0 - s)))).astype(BF16)
        pgq[1, b, r + 1] = pg
        shifted(pgq, b, r + 1, pg.astype(F32))

    @pl.loop(0, frames)
    def _(b):
        for r in range(1, rows - 1):
            through(b, r)
        arrive(2, b)
        through(b, 0)
        through(b, rows - 1)
        send(3, b)

    def ends(buf, b):
        for r in (0, rows + 1):
            shifted(buf, b, r, buf[1, b, r].astype(F32))

    def row_band(get):
        return jnp.concatenate([get(r) for r in range(rows)], axis=1)

    def taps(buf, b):
        return jnp.concatenate(
            [
                row_band(lambda r: buf[q, b, r + 2 - p])
                for p in range(3)
                for q in range(3)
            ],
            axis=0,
        )

    def tap_dot(a, b):
        return lax.dot_general(a, b, (((1,), (1,)), ((), ())), preferred_element_type=F32)

    span = 9 * ch
    width = cin + ch
    low = cin // 128 * 128

    @pl.loop(0, frames)
    def _(b):
        ends(resq, b)
        base = row_band(lambda r: hid[b, r + 1])
        base = jnp.concatenate([jnp.zeros((cin - low, rows * cols), BF16), base], axis=0)
        acc[:span, low:] += tap_dot(taps(resq, b), base)

    @pl.loop(0, frames)
    def _(b):
        arrive(3, b)
        ends(pgq, b)
        base = row_band(lambda r: x[b, r, low:])
        base = jnp.concatenate([base, jnp.zeros((ch, rows * cols), BF16)], axis=0)
        acc[:span, low:] += tap_dot(taps(pgq, b), base)

    def rows_of(index):
        return pl.ds(pl.multiple_of(index * chunk, 8), chunk)

    def remote(src, dst, send_sem, recv_sem, **where):
        return pltpu.make_async_remote_copy(
            src_ref=src, dst_ref=dst, send_sem=send_sem, recv_sem=recv_sem,
            device_id=where, device_id_type=MESH,
        )

    order = [lax.rem(t + k, tiles) for k in range(1, tiles)] + [t]
    arrivals = [lax.rem(t + tiles - k, tiles) for k in range(1, tiles)]
    mine = f * tiles + t
    sends = []

    def start(c):
        c.start()
        sends.append(c)

    def reduction(piece, first, last):
        part = slice(first, last)

        def to_core(d):
            return remote(
                s0.at[d, :, part], r0.at[d, :, part], s0s.at[piece, d], s0r.at[piece, d],
                frame=other,
            )

        def to_tile(d, slot):
            return remote(
                s1.at[d, :, part], r1.at[slot, :, part], s1s.at[piece, d], s1r.at[piece, slot],
                tile=d,
            )

        def result(slot, d, index):
            held = gout.at[slot, :, part]
            return remote(held, held, gs.at[piece, d], gr.at[piece, index], tile=d)

        def across(slot, index):
            held = gout.at[slot, :, part]
            return remote(held, held, ps.at[piece, index], pr.at[piece, index], frame=other)

        def exchange_cores():
            for d in order:
                s0[d, :, part] = acc[rows_of(other * tiles + d), part].astype(BF16)
            for d in order:
                start(to_core(d))

        def scatter():
            for d in order:
                to_core(d).wait_recv()
                v = acc[rows_of(f * tiles + d), part] + r0[d, :, part].astype(F32)
                if d is t:
                    acc[rows_of(mine), part] = v
                else:
                    s1[d, :, part] = v.astype(BF16)
                    start(to_tile(d, t))

        def gather():
            total = acc[rows_of(mine), part]
            for d in arrivals:
                to_tile(d, d).wait_recv()
                total = total + r1[d, :, part].astype(F32)
            gout[mine, :, part] = total.astype(BF16)
            for d in order[:-1]:
                start(result(mine, d, t))
            start(across(mine, t))

        def forward():
            for d in arrivals:
                result(f * tiles + d, d, d).wait_recv()
                start(across(f * tiles + d, d))

        def finish():
            for d in order:
                across(other * tiles + d, d).wait_recv()

        return [exchange_cores, scatter, gather, forward, finish]

    steps = reduction(0, low, width)
    steps.pop(0)()
    for b in range(frames):
        base = row_band(lambda r: x[b, r, :low])
        acc[:span, :low] += tap_dot(taps(pgq, b), base)
        if len(steps) > 1 and b < frames - 1:
            steps.pop(0)()
    last_steps = reduction(1, 0, low)
    last_steps.pop(0)()
    for step in steps + last_steps:
        step()
    for c in sends:
        c.wait_send()


def run_kernel(weights, refs, current, join_kernel, out_kernel, height):
    groups, tiles = lax.axis_size("frame"), lax.axis_size("tile")
    frames, rows, ch, cols = current.shape
    cin = 3 * ch
    count = groups * tiles
    chunk = -(-9 * ch // (count * 8)) * 8
    width = cin + ch
    vm = pl.BlockSpec(memory_space=pltpu.VMEM)
    dma = pltpu.SemaphoreType.DMA
    return pl.pallas_call(
        functools.partial(kernel, groups, tiles, float(height * cols)),
        out_shape=(
            jax.ShapeDtypeStruct((frames, rows, ch, cols), BF16),
            jax.ShapeDtypeStruct((count, chunk, width), BF16),
        ),
        in_specs=[pl.BlockSpec(memory_space=pltpu.SMEM)]
        + [pl.BlockSpec(memory_space=pl.ANY)] * 2
        + [vm] * 2,
        out_specs=(vm, vm),
        scratch_shapes=[
            pltpu.VMEM((frames, rows, cin, cols), BF16),
            pltpu.VMEM((cin, 3 * cin), BF16),
            pltpu.VMEM((cin, cin), BF16),
            pltpu.VMEM((cin, cin), BF16),
            dma((frames, 2)),
            pltpu.VMEM((frames, rows, ch, cols), F32),
            pltpu.VMEM((frames, rows + 2, ch, cols), BF16),
            pltpu.VMEM((3, frames, rows + 2, ch, cols), BF16),
            pltpu.VMEM((3, frames, rows + 2, ch, cols), BF16),
            pltpu.VMEM((2, frames, ch, cols), BF16),
            pltpu.VMEM((2, frames, ch, cols), BF16),
            pltpu.VMEM((count * chunk, width), F32),
        ]
        + [pltpu.VMEM((tiles, chunk, width), BF16)] * 4
        + [dma((4, frames, 2))] * 2
        + [dma((2, tiles))] * 8,
        compiler_params=pltpu.CompilerParams(
            collective_id=0, has_side_effects=True, vmem_limit_bytes=60 * 2**20
        ),
    )(weights, refs, current, join_kernel, out_kernel)


def on_device(
    decoded_refs,
    current_frames,
    ref_pairs,
    ref_slots,
    frame_numbers,
    rate_weights,
    join_kernel,
    out_kernel,
):
    local_refs = decoded_refs.shape[0]
    local_frames, channels, tile_rows, col_count = current_frames.shape
    group = lax.axis_index("frame")
    frame_range = jnp.arange(ref_slots.shape[0], dtype=jnp.int32)

    def pair_slots(which):
        pairs = lax.dynamic_slice_in_dim(ref_pairs, which * local_frames, local_frames, 0)
        return jnp.sum(jnp.where(pairs[:, :, None] == frame_range, ref_slots, 0), axis=-1).reshape(
            -1
        )

    mine = pair_slots(group)
    other = pair_slots(1 - group) - group * local_refs
    outgoing = jnp.take(decoded_refs, jnp.clip(other, 0, local_refs - 1), axis=0, mode="clip")
    incoming = partner(outgoing, "frame", 0)
    mine_local = mine - group * local_refs
    mine_held = (mine_local >= 0) & (mine_local < local_refs)
    own_tiles = jnp.take(decoded_refs, jnp.clip(mine_local, 0, local_refs - 1), axis=0, mode="clip")
    picked = jnp.where(mine_held[:, None, None, None], own_tiles, incoming)
    picked = picked.reshape(local_frames, 2 * channels, tile_rows, col_count)
    refs = picked.transpose(0, 2, 1, 3)
    current = current_frames.transpose(0, 2, 1, 3)
    height = tile_rows * lax.axis_size("tile")

    frames_here = lax.dynamic_slice_in_dim(frame_numbers, group * local_frames, local_frames, 0)
    gop_range = jnp.arange(rate_weights.shape[0], dtype=jnp.int32)
    weight_here = jnp.sum(jnp.where(frames_here[:, None] == gop_range, rate_weights, 0.0), axis=-1)

    recon, grads = run_kernel(weight_here, refs, current, join_kernel, out_kernel, height)
    grads = grads.reshape(-1, 4 * channels)
    inputs = 3 * channels
    join_total = grads[: 9 * channels, :inputs].astype(F32).reshape(join_kernel.shape)
    output_total = grads[: 9 * channels, inputs:].astype(F32).reshape(out_kernel.shape)
    return (recon.transpose(0, 2, 1, 3), join_total, output_total)


def solution(mesh):
    placed = (
        P(("parts", "frame"), None, "tile", None),
        P(("parts", "frame"), None, "tile", None),
        P("parts", None),
        P("parts"),
        P("parts"),
        P("parts"),
        P(),
        P(),
    )
    return jax.shard_map(
        on_device,
        mesh=mesh,
        in_specs=placed,
        out_specs=(
            P(("parts", "frame"), None, "tile", None),
            P("parts", None, None, None),
            P("parts", None, None, None),
        ),
        check_vma=False,
    )
```

```python
import functools

import jax
import jax.numpy as jnp
from jax import lax
from jax.experimental import pallas as pl
from jax.experimental.pallas import tpu as pltpu
from jax.sharding import PartitionSpec as P

MESH = pl.DeviceIdType.MESH
BF16 = jnp.bfloat16
F32 = jnp.float32


def partner(array, axis, stride):
    return lax.ppermute(array, axis, [(i, i ^ 1 << stride) for i in range(lax.axis_size(axis))])


def dot(a, b):
    return jnp.dot(a, b, preferred_element_type=F32)


def from_left(v):
    lane = lax.broadcasted_iota(jnp.int32, v.shape, 1)
    return jnp.where(lane == 0, 0.0, pltpu.roll(v, 1, 1))


def from_right(v):
    cols = v.shape[1]
    lane = lax.broadcasted_iota(jnp.int32, v.shape, 1)
    return jnp.where(lane == cols - 1, 0.0, pltpu.roll(v, cols - 1, 1))


def join_cols(v, ch):
    return from_left(v[:ch]) + v[ch : 2 * ch] + from_right(v[2 * ch :])


def kernel(
    groups, tiles, scale_cells, wt, refs, current, kj_in, ko_in,
    recon_out, gout,
    x, kj, ko, kt, in_sem, pre, hid, resq, pgq, part_s, part_r, acc, acc_o, s0, r0, s1, r1,
    hs, hr, s0s, s0r, s1s, s1r, gs, gr, ps, pr,
):
    frames, rows, cin, cols = x.shape
    ch = cin // 3
    chunk = gout.shape[1]
    f = lax.axis_index("frame")
    t = lax.axis_index("tile")
    other = 1 - f
    has_up = t > 0
    has_down = t < tiles - 1

    def load(b):
        return (
            pltpu.make_async_copy(refs.at[b], x.at[b, :, : 2 * ch], in_sem.at[b, 0]),
            pltpu.make_async_copy(current.at[b], x.at[b, :, 2 * ch :], in_sem.at[b, 1]),
        )

    for b in range(frames):
        for c in load(b):
            c.start()

    barrier = pltpu.get_barrier_semaphore()
    pl.semaphore_signal(barrier, inc=1, device_id={"frame": other}, device_id_type=MESH)
    for k in range(1, tiles):
        pl.semaphore_signal(
            barrier, inc=1, device_id={"tile": lax.rem(t + k, tiles)}, device_id_type=MESH
        )
    pl.semaphore_wait(barrier, tiles)

    def exchange(stage, b):
        if stage == 0:
            to_up, up_slot = part_s.at[0, b], part_r.at[1, b]
            to_down, down_slot = part_s.at[1, b], part_r.at[0, b]
        else:
            buf = (hid, resq.at[1], pgq.at[1])[stage - 1]
            to_up, up_slot = buf.at[b, 1], buf.at[b, rows + 1]
            to_down, down_slot = buf.at[b, rows], buf.at[b, 0]
        up = pltpu.make_async_remote_copy(
            src_ref=to_up, dst_ref=up_slot,
            send_sem=hs.at[stage, b, 0], recv_sem=hr.at[stage, b, 0],
            device_id={"tile": lax.max(t - 1, 0)}, device_id_type=MESH,
        )
        down = pltpu.make_async_remote_copy(
            src_ref=to_down, dst_ref=down_slot,
            send_sem=hs.at[stage, b, 1], recv_sem=hr.at[stage, b, 1],
            device_id={"tile": lax.min(t + 1, tiles - 1)}, device_id_type=MESH,
        )
        return up, down

    def send(stage, b):
        up, down = exchange(stage, b)

        @pl.when(has_up)
        def _():
            up.start()

        @pl.when(has_down)
        def _():
            down.start()

    def arrive(stage, b):
        up, down = exchange(stage, b)

        @pl.when(has_up)
        def _():
            down.wait_recv()
            up.wait_send()

        @pl.when(has_down)
        def _():
            up.wait_recv()
            down.wait_send()

    edge = jnp.zeros((frames, ch, cols), BF16)

    @pl.when(jnp.logical_not(has_up))
    def _():
        part_r[0] = edge
        hid[:, 0] = edge
        resq[1, :, 0] = edge
        pgq[1, :, 0] = edge

    @pl.when(jnp.logical_not(has_down))
    def _():
        part_r[1] = edge
        hid[:, rows + 1] = edge
        resq[1, :, rows + 1] = edge
        pgq[1, :, rows + 1] = edge

    for p in range(3):
        for q in range(3):
            kj[q * ch : (q + 1) * ch, p * cin : (p + 1) * cin] = kj_in[p, q]
            ko[q * ch : (q + 1) * ch, p * ch : (p + 1) * ch] = ko_in[p, q]
            flipped = ko_in[2 - p, 2 - q].astype(F32).T.astype(BF16)
            kt[q * ch : (q + 1) * ch, p * ch : (p + 1) * ch] = flipped

    @pl.loop(0, frames)
    def _(b):
        for c in load(b):
            c.wait()
        part_s[0, b] = join_cols(dot(kj[:, 2 * cin :], x[b, 0]), ch).astype(BF16)
        part_s[1, b] = join_cols(dot(kj[:, :cin], x[b, rows - 1]), ch).astype(BF16)
        send(0, b)

    acc[...] = jnp.zeros_like(acc)
    acc_o[...] = jnp.zeros_like(acc_o)

    def activate(b, r, v):
        pre[b, r] = v
        hid[b, r + 1] = (v * jax.nn.sigmoid(v)).astype(BF16)

    @pl.loop(0, frames)
    def _(b):
        pre[b, 0] = join_cols(dot(kj[:, cin:], x[b, 0:2].reshape(2 * cin, cols)), ch)
        pre[b, rows - 1] = join_cols(
            dot(kj[:, : 2 * cin], x[b, rows - 2 : rows].reshape(2 * cin, cols)), ch
        )
        for r in range(1, rows - 1):
            v = join_cols(dot(kj[...], x[b, r - 1 : r + 2].reshape(3 * cin, cols)), ch)
            activate(b, r, v)
        arrive(0, b)
        activate(b, 0, pre[b, 0] + part_r[0, b].astype(F32))
        activate(b, rows - 1, pre[b, rows - 1] + part_r[1, b].astype(F32))
        send(1, b)

    def shifted(buf, b, r, v):
        buf[0, b, r] = from_right(v).astype(BF16)
        buf[2, b, r] = from_left(v).astype(BF16)

    def reconstruct(b, r):
        v = join_cols(dot(ko[...], hid[b, r : r + 3].reshape(3 * ch, cols)), ch)
        recon_out[b, r] = v.astype(BF16)
        target = x[b, r, 2 * ch :].astype(F32)
        res = (2.0 * wt[b] * (v - target) / scale_cells).astype(BF16)
        resq[1, b, r + 1] = res
        shifted(resq, b, r + 1, res.astype(F32))

    @pl.loop(0, frames)
    def _(b):
        for r in range(1, rows - 1):
            reconstruct(b, r)
        arrive(1, b)
        reconstruct(b, 0)
        reconstruct(b, rows - 1)
        send(2, b)

    def through(b, r):
        hg = join_cols(dot(kt[...], resq[1, b, r : r + 3].reshape(3 * ch, cols)), ch)
        v = pre[b, r]
        s = jax.nn.sigmoid(v)
        pg = (hg * (s * (1.0 + v * (1.0 - s)))).astype(BF16)
        pgq[1, b, r + 1] = pg
        shifted(pgq, b, r + 1, pg.astype(F32))

    @pl.loop(0, frames)
    def _(b):
        for r in range(1, rows - 1):
            through(b, r)
        arrive(2, b)
        through(b, 0)
        through(b, rows - 1)
        send(3, b)

    def ends(buf, b):
        for r in (0, rows + 1):
            shifted(buf, b, r, buf[1, b, r].astype(F32))

    def row_band(get):
        return jnp.concatenate([get(r) for r in range(rows)], axis=1)

    def taps(buf, b):
        return jnp.concatenate(
            [
                row_band(lambda r: buf[q, b, r + 2 - p])
                for p in range(3)
                for q in range(3)
            ],
            axis=0,
        )

    def tap_dot(a, b):
        return lax.dot_general(a, b, (((1,), (1,)), ((), ())), preferred_element_type=F32)

    span = 9 * ch

    @pl.loop(0, frames)
    def _(b):
        ends(resq, b)
        base = row_band(lambda r: hid[b, r + 1])
        acc_o[...] += tap_dot(base, taps(resq, b))

    @pl.loop(0, frames)
    def _(b):
        arrive(3, b)
        ends(pgq, b)
        base = row_band(lambda r: x[b, r])
        acc[:span, :cin] += tap_dot(taps(pgq, b), base)

    for k in range(9):
        acc[k * ch : (k + 1) * ch, cin:] = acc_o[:, k * ch : (k + 1) * ch].T

    def rows_of(index):
        return pl.ds(pl.multiple_of(index * chunk, 8), chunk)

    def remote(src, dst, send, recv, **where):
        return pltpu.make_async_remote_copy(
            src_ref=src, dst_ref=dst, send_sem=send, recv_sem=recv,
            device_id=where, device_id_type=MESH,
        )

    order = [lax.rem(t + k, tiles) for k in range(1, tiles)] + [t]
    sends = []
    for d in order:
        s0[d] = acc[rows_of(other * tiles + d)].astype(BF16)
    for d in order:
        c = remote(s0.at[d], r0.at[d], s0s.at[d], s0r.at[d], frame=other)
        c.start()
        sends.append(c)
    total = None
    for i, d in enumerate(order):
        sends[i].wait_recv()
        v = acc[rows_of(f * tiles + d)] + r0[d].astype(F32)
        if i == tiles - 1:
            total = v
            break
        s1[d] = v.astype(BF16)
        c = remote(s1.at[d], r1.at[t], s1s.at[d], s1r.at[t], tile=d)
        c.start()
        sends.append(c)
    for d in order[:-1]:
        remote(s1.at[d], r1.at[d], s1s.at[d], s1r.at[d], tile=d).wait_recv()
        total = total + r1[d].astype(F32)
    mine = f * tiles + t
    gout[mine] = total.astype(BF16)
    for d in order[:-1]:
        c = remote(gout.at[mine], gout.at[mine], gs.at[d], gr.at[t], tile=d)
        c.start()
        sends.append(c)
    across = []
    for d in [t] + [lax.rem(t + tiles - k, tiles) for k in range(1, tiles)]:
        slot = f * tiles + d
        if across:
            remote(gout.at[slot], gout.at[slot], gs.at[d], gr.at[d], tile=d).wait_recv()
        c = remote(gout.at[slot], gout.at[slot], ps.at[d], pr.at[d], frame=other)
        c.start()
        across.append(c)
        sends.append(c)
    for d in order:
        slot = other * tiles + d
        remote(gout.at[slot], gout.at[slot], ps.at[d], pr.at[d], frame=other).wait_recv()
    for c in sends:
        c.wait_send()


def run_kernel(weights, refs, current, join_kernel, out_kernel, height):
    groups, tiles = lax.axis_size("frame"), lax.axis_size("tile")
    frames, rows, ch, cols = current.shape
    cin = 3 * ch
    count = groups * tiles
    chunk = -(-9 * ch // (count * 8)) * 8
    width = cin + ch
    vm = pl.BlockSpec(memory_space=pltpu.VMEM)
    dma = pltpu.SemaphoreType.DMA
    return pl.pallas_call(
        functools.partial(kernel, groups, tiles, float(height * cols)),
        out_shape=(
            jax.ShapeDtypeStruct((frames, rows, ch, cols), BF16),
            jax.ShapeDtypeStruct((count, chunk, width), BF16),
        ),
        in_specs=[pl.BlockSpec(memory_space=pltpu.SMEM)]
        + [pl.BlockSpec(memory_space=pl.ANY)] * 2
        + [vm] * 2,
        out_specs=(vm, vm),
        scratch_shapes=[
            pltpu.VMEM((frames, rows, cin, cols), BF16),
            pltpu.VMEM((cin, 3 * cin), BF16),
            pltpu.VMEM((cin, cin), BF16),
            pltpu.VMEM((cin, cin), BF16),
            dma((frames, 2)),
            pltpu.VMEM((frames, rows, ch, cols), F32),
            pltpu.VMEM((frames, rows + 2, ch, cols), BF16),
            pltpu.VMEM((3, frames, rows + 2, ch, cols), BF16),
            pltpu.VMEM((3, frames, rows + 2, ch, cols), BF16),
            pltpu.VMEM((2, frames, ch, cols), BF16),
            pltpu.VMEM((2, frames, ch, cols), BF16),
            pltpu.VMEM((count * chunk, width), F32),
            pltpu.VMEM((ch, 9 * ch), F32),
        ]
        + [pltpu.VMEM((tiles, chunk, width), BF16)] * 4
        + [dma((4, frames, 2))] * 2
        + [dma((tiles,))] * 8,
        compiler_params=pltpu.CompilerParams(
            collective_id=0, has_side_effects=True, vmem_limit_bytes=60 * 2**20
        ),
    )(weights, refs, current, join_kernel, out_kernel)


def on_device(
    decoded_refs,
    current_frames,
    ref_pairs,
    ref_slots,
    frame_numbers,
    rate_weights,
    join_kernel,
    out_kernel,
):
    local_refs = decoded_refs.shape[0]
    local_frames, channels, tile_rows, col_count = current_frames.shape
    group = lax.axis_index("frame")
    frame_range = jnp.arange(ref_slots.shape[0], dtype=jnp.int32)

    def pair_slots(which):
        pairs = lax.dynamic_slice_in_dim(ref_pairs, which * local_frames, local_frames, 0)
        return jnp.sum(jnp.where(pairs[:, :, None] == frame_range, ref_slots, 0), axis=-1).reshape(
            -1
        )

    mine = pair_slots(group)
    other = pair_slots(1 - group) - group * local_refs
    outgoing = jnp.take(decoded_refs, jnp.clip(other, 0, local_refs - 1), axis=0, mode="clip")
    incoming = partner(outgoing, "frame", 0)
    mine_local = mine - group * local_refs
    mine_held = (mine_local >= 0) & (mine_local < local_refs)
    own_tiles = jnp.take(decoded_refs, jnp.clip(mine_local, 0, local_refs - 1), axis=0, mode="clip")
    picked = jnp.where(mine_held[:, None, None, None], own_tiles, incoming)
    picked = picked.reshape(local_frames, 2 * channels, tile_rows, col_count)
    refs = picked.transpose(0, 2, 1, 3)
    current = current_frames.transpose(0, 2, 1, 3)
    height = tile_rows * lax.axis_size("tile")

    frames_here = lax.dynamic_slice_in_dim(frame_numbers, group * local_frames, local_frames, 0)
    gop_range = jnp.arange(rate_weights.shape[0], dtype=jnp.int32)
    weight_here = jnp.sum(jnp.where(frames_here[:, None] == gop_range, rate_weights, 0.0), axis=-1)

    recon, grads = run_kernel(weight_here, refs, current, join_kernel, out_kernel, height)
    grads = grads.reshape(-1, 4 * channels)[: 9 * channels].astype(F32)
    grads = grads.reshape(3, 3, channels, 4 * channels)
    return (
        recon.transpose(0, 2, 1, 3),
        grads[..., : 3 * channels],
        grads[..., 3 * channels :],
    )


def solution(mesh):
    placed = (
        P(("parts", "frame"), None, "tile", None),
        P(("parts", "frame"), None, "tile", None),
        P("parts", None),
        P("parts"),
        P("parts"),
        P("parts"),
        P(),
        P(),
    )
    return jax.shard_map(
        on_device,
        mesh=mesh,
        in_specs=placed,
        out_specs=(
            P(("parts", "frame"), None, "tile", None),
            P("parts", None, None, None),
            P("parts", None, None, None),
        ),
        check_vma=False,
    )
```
